32 devices in a mesh: dp: 8 (over y, x, core), mp: 4 (over z).
Axes of the slice: x: 2, y: 2, z: 4, core: 2. Of those that a mesh axis runs over, the one named last changes fastest.
Arguments:
- tokens: bfloat16 [12288, 4096], P('dp'), may hold values from -40 to 40
- norm_gain: bfloat16 [4096], replicated, may hold values from 0.099609375 to 1.8984375
- w_query: bfloat16 [4096, 2048], P(None, 'mp'), may hold values from -1 to 1
- w_key: bfloat16 [4096, 512], P(None, 'mp'), may hold values from -4 to 4
- w_value: bfloat16 [4096, 512], P(None, 'mp'), may hold values from -0.09375 to 0.09375
- w_out: bfloat16 [2048, 4096], P('mp'), may hold values from -0.125 to 0.125
- seq_starts: int32 [64], P('dp'), may hold values from 0 to 1408, as said below
- seq_lengths: int32 [64], P('dp'), may hold values from 128 to 640
- episode_ids: int32 [64], replicated, may hold values from 0 to 0, as said below
- class_ids: int32 [64], replicated, may hold values from 0 to 31
- query_flags: int32 [64], replicated, may hold values from 0 to 1
Outputs:
- log_probs: float32 [64, 32], P('dp')
- prototypes: float32 [32, 4096], P(None, 'mp')
The draws below stay inside these ranges and needn't reach their ends.
Inputs may be any that keep to these rules, and one draw needn't show every extreme that they name: `seq_starts`: slot s lies in the buffer of dp index s // 8; the slots of one buffer are disjoint and in increasing order of start; start plus length is at most 1536, and in every draw the last slot of some buffer ends at row 1536. `episode_ids`: every class of every episode has at least one support sequence.
All inputs are finite; a program needn't handle non-finite values.
Results may differ from the reference program's by a relative error of at most 0.004.
Values sent between devices are 32-bit elements; how exact they have to be, the bound alone decides.
A program may use at most 128 MiB of HBM per device.

```python
import math
import jax
import jax.numpy as jnp
from jax import lax

D = 4096
HEAD_DIM = 128
HEADS = 16
KV_HEADS = 4
WAYS = 32
MIN_LEN = 128
SEQ_DEV = 8
CAP = 1536
NSEQ = 64
EPISODES = 1
CLASSES = 32


def packing(key):
    groups = NSEQ // SEQ_DEV
    subkeys = jax.random.split(jax.random.fold_in(key, 13), 4)
    spare_tokens = CAP - SEQ_DEV * MIN_LEN
    filled = jax.random.randint(subkeys[0], (groups,), 0, spare_tokens + 1)
    fullest = jax.random.randint(subkeys[1], (), 0, groups)
    filled = jnp.where(jnp.arange(groups) == fullest, spare_tokens, filled)
    raw_weights = jax.random.randint(subkeys[2], (groups, 2 * SEQ_DEV), 1, 17)
    weights = raw_weights * raw_weights * raw_weights
    shares = filled[:, None] * weights // jnp.sum(weights, axis=1, keepdims=True)
    remain = filled - jnp.sum(shares, axis=1)
    shares = shares.at[:, 0].add(remain)
    longest_slot = jax.random.randint(subkeys[3], (), 0, SEQ_DEV)
    single = jnp.where(jnp.arange(2 * SEQ_DEV) == longest_slot, spare_tokens, 0)
    shares = jnp.where((jnp.arange(groups) == fullest)[:, None], single[None, :], shares)
    lengths = MIN_LEN + shares[:, :SEQ_DEV]
    gap_sizes = shares[:, SEQ_DEV:]
    extents = lengths + gap_sizes
    starts = jnp.cumsum(extents, axis=1) - extents + gap_sizes
    return (starts.reshape(-1).astype(jnp.int32), lengths.reshape(-1).astype(jnp.int32))


def draw_seq_starts(key, part):
    return packing(key)[0]


def draw_seq_lengths(key, part):
    return packing(key)[1]


def labels(key):
    subkeys = jax.random.split(jax.random.fold_in(key, 7), 3)
    slot_index = jnp.arange(NSEQ, dtype=jnp.int32)
    extra_class = jax.random.randint(subkeys[0], (NSEQ,), 0, CLASSES)
    global_class = jnp.where(slot_index < CLASSES, slot_index, extra_class)
    coin = jax.random.randint(subkeys[1], (NSEQ,), 0, 2)
    asked_flag = jnp.where(slot_index < CLASSES, 0, jnp.where(slot_index == CLASSES, 1, coin))
    shuffle = jax.random.permutation(subkeys[2], NSEQ)
    return (global_class[shuffle], asked_flag[shuffle])


def draw_episode_ids(key, part):
    return (labels(key)[0] // WAYS).astype(jnp.int32)


def draw_class_ids(key, part):
    return (labels(key)[0] % WAYS).astype(jnp.int32)


def draw_query_flags(key, part):
    return labels(key)[1].astype(jnp.int32)


def query_key_pair(key):
    subkeys = jax.random.split(jax.random.fold_in(key, 21), 2)
    query_weight = jax.random.normal(subkeys[0], (D, HEADS * HEAD_DIM), jnp.float32) / math.sqrt(D)
    key_weight = jax.random.normal(subkeys[1], (D, KV_HEADS * HEAD_DIM), jnp.float32) / math.sqrt(D)
    return (jnp.clip(query_weight, -1.0, 1.0), jnp.clip(key_weight, -4.0, 4.0))


def draw_w_query(key, part):
    return query_key_pair(key)[0].astype(jnp.bfloat16)


def draw_w_key(key, part):
    return query_key_pair(key)[1].astype(jnp.bfloat16)


def draw_tokens(key, part):
    row_total = NSEQ // SEQ_DEV * CAP
    subkeys = jax.random.split(jax.random.fold_in(key, 31), 1)
    values = jax.random.normal(subkeys[0], (row_total, D), jnp.float32)
    values = jnp.clip(values, -6.0, 6.0)
    return values.astype(jnp.bfloat16)


def levels(own_key, shape, pieces, smallest, largest):
    level, own = 1.0, jax.random.fold_in(own_key, 6)
    for dim, parts in pieces:
        draws = jnp.exp(jax.random.uniform(jax.random.fold_in(own, dim), (parts,), jnp.float32, smallest / len(pieces), largest / len(pieces)))
        level = level * jnp.repeat(draws, shape[dim] // parts).reshape([-1 if axis == dim else 1 for axis in range(len(shape))])
    return level


def gaussian(key, shape, spread, most, shards=(), kind=jnp.bfloat16):
    entries = spread * jax.random.normal(key, shape, jnp.float32)
    if shards:
        entries = entries * levels(key, shape, shards, -0.22, 0.18)
    return jnp.clip(entries, -most, most).astype(kind)


def setup_inputs(seed: int = 0) -> dict:
    seeds = jax.random.split(jax.random.key(seed), 12)
    return {
        "tokens": draw_tokens(jax.random.fold_in(seeds[11], 71), 0),
        "norm_gain": jnp.clip(1.0 + 0.18 * jax.random.normal(seeds[1], (D,), jnp.float32), 0.099609375, 1.8984375).astype(jnp.bfloat16),
        "w_query": draw_w_query(jax.random.fold_in(seeds[11], 71), 0),
        "w_key": draw_w_key(jax.random.fold_in(seeds[11], 71), 0),
        "w_value": gaussian(seeds[4], (D, KV_HEADS * HEAD_DIM), D ** -0.5, 0.09375, ((1, 4),)),
        "w_out": gaussian(seeds[5], (HEADS * HEAD_DIM, D), (HEADS * HEAD_DIM) ** -0.5, 0.125, ((0, 4),)),
        "seq_starts": draw_seq_starts(jax.random.fold_in(seeds[11], 71), 0),
        "seq_lengths": draw_seq_lengths(jax.random.fold_in(seeds[11], 71), 0),
        "episode_ids": draw_episode_ids(jax.random.fold_in(seeds[11], 71), 0),
        "class_ids": draw_class_ids(jax.random.fold_in(seeds[11], 71), 0),
        "query_flags": draw_query_flags(jax.random.fold_in(seeds[11], 71), 0),
    }


ROPE_BASE = 500000.0
NEG_FILL = -1e+30

def rotate(vectors, positions):
    half_dim = vectors.shape[-1] // 2
    frequency = jnp.power(ROPE_BASE, -(jnp.arange(half_dim, dtype=jnp.float32) * 2.0 / vectors.shape[-1]))
    angles = positions.astype(jnp.float32)[:, None] * frequency[None, :]
    cosine = jnp.cos(angles)[:, None, :]
    sine_part = jnp.sin(angles)[:, None, :]
    leading = vectors[..., :half_dim]
    trailing = vectors[..., half_dim:]
    return jnp.concatenate([leading * cosine - trailing * sine_part, trailing * cosine + leading * sine_part], axis=-1)

def layout_of(starts, lengths, buffer_len):
    token_index = jnp.arange(buffer_len, dtype=jnp.int32)
    inside = (token_index[:, None] >= starts[None, :]) & (token_index[:, None] < (starts + lengths)[None, :])
    slot_number = jnp.arange(starts.shape[0], dtype=jnp.int32)
    segment = lax.optimization_barrier(jnp.sum(jnp.where(inside, slot_number[None, :] + 1, 0), axis=1)).astype(jnp.int32) - 1
    position = lax.optimization_barrier(jnp.sum(jnp.where(inside, token_index[:, None] - starts[None, :], 0), axis=1)).astype(jnp.int32)
    return (segment, position, inside)

def allowed_mask(segment, row_start, row_count, col_count):
    rows_index = row_start + jnp.arange(row_count, dtype=jnp.int32)
    cols_index = jnp.arange(col_count, dtype=jnp.int32)
    seg_rows = segment[row_start:row_start + row_count]
    seg_cols = segment[:col_count]
    same = (seg_rows[:, None] == seg_cols[None, :]) & (seg_rows[:, None] >= 0) & (cols_index[None, :] < rows_index[:, None])
    return (rows_index[:, None] == cols_index[None, :]) | same

def softmax_rows(scores, permitted):
    masked_scores = jnp.where(permitted[None, None], scores, NEG_FILL)
    row_peak = lax.optimization_barrier(jnp.max(masked_scores, axis=-1, keepdims=True))
    exponent = jnp.exp(masked_scores - row_peak)
    totals = lax.optimization_barrier(jnp.sum(exponent, axis=-1, keepdims=True))
    return (exponent / totals).astype(jnp.bfloat16)

def reference(tokens, norm_gain, w_query, w_key, w_value, w_out, seq_starts, seq_lengths, episode_ids, class_ids, query_flags):
    group_count = NSEQ // SEQ_DEV
    group_size = HEADS // KV_HEADS
    inv_root = 1.0 / math.sqrt(HEAD_DIM)
    highest = lax.Precision.HIGHEST

    def embed_group(row_items):
        buffer_rows, starts, lengths = row_items
        segment, position, inside = layout_of(starts, lengths, CAP)
        widened = buffer_rows.astype(jnp.float32)
        normed = (widened * lax.rsqrt(lax.optimization_barrier(jnp.mean(widened * widened, axis=-1, keepdims=True)) + 1e-05) * norm_gain.astype(jnp.float32)).astype(jnp.bfloat16)
        queries = rotate(jnp.dot(normed, w_query, preferred_element_type=jnp.float32).reshape(CAP, HEADS, HEAD_DIM), position).astype(jnp.bfloat16)
        queries = queries.reshape(CAP, KV_HEADS, group_size, HEAD_DIM)
        keys_rot = rotate(jnp.dot(normed, w_key, preferred_element_type=jnp.float32).reshape(CAP, KV_HEADS, HEAD_DIM), position).astype(jnp.bfloat16)
        values_all = jnp.dot(normed, w_value, preferred_element_type=jnp.float32).astype(jnp.bfloat16).reshape(CAP, KV_HEADS, HEAD_DIM)
        scores = jnp.einsum('qngd,knd->ngqk', queries.astype(jnp.float32), keys_rot.astype(jnp.float32), precision=highest) * inv_root
        permitted = allowed_mask(segment, 0, CAP, CAP)
        attention_probs = softmax_rows(scores, permitted)
        attended = jnp.einsum('ngqk,knd->qngd', attention_probs.astype(jnp.float32), values_all.astype(jnp.float32), precision=highest)
        attended = attended.astype(jnp.bfloat16).reshape(CAP, HEADS * HEAD_DIM)
        layer_out = widened + jnp.dot(attended, w_out, preferred_element_type=jnp.float32)
        member = inside.T.astype(jnp.float32)
        return jnp.dot(member, layer_out, precision=highest) / lengths.astype(jnp.float32)[:, None]
    pooled = lax.map(embed_group, (tokens.reshape(group_count, CAP, D), seq_starts.reshape(group_count, SEQ_DEV), seq_lengths.reshape(group_count, SEQ_DEV)))
    pooled = pooled.reshape(NSEQ, D)
    embedded = pooled * lax.rsqrt(lax.optimization_barrier(jnp.mean(pooled * pooled, axis=-1, keepdims=True)) + 1e-06)
    global_class = episode_ids * WAYS + class_ids
    is_support = query_flags == 0
    select_all = ((global_class[None, :] == jnp.arange(CLASSES, dtype=jnp.int32)[:, None]) & is_support[None, :]).astype(jnp.float32)
    class_sums = jnp.dot(select_all, embedded, precision=highest)
    prototypes = class_sums * lax.rsqrt(lax.optimization_barrier(jnp.mean(class_sums * class_sums, axis=-1, keepdims=True)) + 1e-06)
    episode_protos = prototypes.reshape(EPISODES, WAYS, D)

    def score_row(row_items):
        vector, episode = row_items
        chosen = lax.dynamic_index_in_dim(episode_protos, episode, 0, keepdims=False)
        difference = vector[None, :] - chosen
        return lax.optimization_barrier(jnp.sum(difference * difference, axis=-1))
    distance = lax.map(score_row, (embedded, episode_ids))
    logits = -distance / math.sqrt(D)
    row_peak = lax.optimization_barrier(jnp.max(logits, axis=-1, keepdims=True))
    shifted = logits - row_peak
    log_probs = shifted - jnp.log(lax.optimization_barrier(jnp.sum(jnp.exp(shifted), axis=-1, keepdims=True)))
    log_probs = jnp.where(query_flags[:, None] == 1, log_probs, 0.0)
    return (log_probs, prototypes)
```

```python
import functools
import math

import numpy as np
import jax
import jax.numpy as jnp
from jax import lax
from jax.experimental import pallas as pl
from jax.experimental.pallas import tpu as pltpu
from jax.sharding import PartitionSpec as P

HEAD_DIM = 128
WAYS = 32
ROPE_BASE = 500000.0
NEG_FILL = -1e30
MESH = pl.DeviceIdType.MESH
F32 = jnp.float32
BF16 = jnp.bfloat16
HIGHEST = lax.Precision.HIGHEST


def pick(total, options):
    for candidate in options:
        if total % candidate == 0:
            return candidate
    return total


def encode_kernel(
    dims, st_ref, ln_ref, x_ref, gain_ref, wq_hbm, wk_hbm, wv_hbm, wo_hbm, cos_ref, sin_ref,
    hp_ref, ts_ref, w_s, wo_s, q_s, k_s, v_s, s_s, c_s, w_sem, wo_sem,
):
    rows, tile, qb, width, slots, heads, chunk, share, n_mp = dims
    hd = HEAD_DIM
    i = pl.program_id(0)
    last = pl.num_programs(0) - 1
    q_cols = heads * hd
    chunks = width // chunk
    rank = lax.axis_index("mp")
    wo_copy = pltpu.make_async_copy(wo_hbm, wo_s, wo_sem)

    def members(first, count):
        slot = lax.broadcasted_iota(jnp.int32, (slots, count), 0)
        token = lax.broadcasted_iota(jnp.int32, (slots, count), 1) + first
        lo = jnp.zeros((slots, count), jnp.int32)
        hi = jnp.zeros((slots, count), jnp.int32)
        for j in range(slots):
            lo = jnp.where(slot == j, st_ref[j], lo)
            hi = jnp.where(slot == j, st_ref[j] + ln_ref[j], hi)
        return jnp.where((token >= lo) & (token < hi), 1.0, 0.0).astype(BF16)

    @pl.when(i == 0)
    def _():
        def copies(c):
            r = pl.ds(c * chunk, chunk)
            return (
                pltpu.make_async_copy(wq_hbm.at[r, :], w_s.at[r, pl.ds(0, q_cols)], w_sem.at[c, 0]),
                pltpu.make_async_copy(wk_hbm.at[r, :], w_s.at[r, pl.ds(q_cols, hd)], w_sem.at[c, 1]),
                pltpu.make_async_copy(wv_hbm.at[r, :], w_s.at[r, pl.ds(q_cols + hd, hd)], w_sem.at[c, 2]),
            )

        for c in range(chunks):
            for copy in copies(c):
                copy.start()
        wo_copy.start()
        ts_ref[...] = jnp.zeros_like(ts_ref)
        c_s[...] = jnp.zeros_like(c_s)
        for c in range(chunks):
            for copy in copies(c):
                copy.wait()
            for b in range(chunk // 128):
                at = c * chunk + b * 128
                g = jnp.broadcast_to(gain_ref[:, at : at + 128].astype(F32), (128, 128)).T
                for v in range(heads + 2):
                    w = w_s[at : at + 128, v * hd : (v + 1) * hd].astype(F32)
                    w_s[at : at + 128, v * hd : (v + 1) * hd] = (w * g).astype(BF16)

    half = tile // 2
    sums = []
    for b in range(2):
        acc = jnp.zeros((half, 128), F32)
        for v in range(width // 128):
            x = x_ref[b * half : (b + 1) * half, v * 128 : (v + 1) * 128].astype(F32)
            acc = acc + x * x
        sums.append(jnp.sum(acc, axis=-1, keepdims=True))
    rstd = lax.rsqrt(jnp.concatenate(sums, axis=0) / width + 1e-05)
    proj = jnp.dot(x_ref[...], w_s[...], preferred_element_type=F32)
    cos = cos_ref[...]
    sin = sin_ref[...]

    def rope(y):
        return (y * cos + pltpu.roll(y, hd // 2, 1) * sin).astype(BF16)

    q_rstd = rstd * (math.log2(math.e) / math.sqrt(hd))
    for h in range(heads):
        q_s[h] = rope(proj[:, h * hd : (h + 1) * hd] * q_rstd)
    here = pl.ds(pl.multiple_of(i * tile, tile), tile)
    k_s[here, :] = rope(proj[:, q_cols : q_cols + hd] * rstd)
    v_s[here, :] = (proj[:, q_cols + hd :] * rstd).astype(BF16)
    cols = pl.ds(pl.multiple_of(rank * share, share), share)
    ts_ref[...] += jnp.dot(members(i * tile, tile), x_ref[:, cols], preferred_element_type=F32)

    for b in range(tile // qb):
        block = i * (tile // qb) + b
        first = block * qb
        lo_row = first
        token = lax.broadcasted_iota(jnp.int32, (1, qb), 1) + first
        start = token
        for j in range(slots):
            s0 = st_ref[j]
            s1 = s0 + ln_ref[j]
            start = jnp.where((token >= s0) & (token < s1), s0, start)
            lo_row = jnp.where((first >= s0) & (first < s1), s0, lo_row)
        lo = lo_row // qb

        def fold(a, op):
            return op(a.reshape(qb // 8, 8, qb), axis=0)

        def score(kb, peaks):
            at = pl.ds(pl.multiple_of(kb * qb, qb), qb)
            keys = k_s[at, :]
            row = lax.broadcasted_iota(jnp.int32, (qb, qb), 0) + kb * qb
            ok = (row >= start) & (row <= token)
            out = []
            for h in range(heads):
                s = lax.dot_general(
                    keys, q_s[h, b * qb : (b + 1) * qb, :], (((1,), (1,)), ((), ())),
                    preferred_element_type=F32,
                )
                s = jnp.where(ok, s, NEG_FILL)
                s_s[at, h * qb : (h + 1) * qb] = s
                out.append(jnp.maximum(peaks[h], fold(s, jnp.max)))
            return tuple(out)

        peaks = lax.fori_loop(
            lo, block + 1, score, tuple(jnp.full((8, qb), NEG_FILL, F32) for _ in range(heads))
        )
        peaks = [jnp.max(p, axis=0, keepdims=True) for p in peaks]

        def expo(kb, totals):
            at = pl.ds(pl.multiple_of(kb * qb, qb), qb)
            out = []
            for h in range(heads):
                e = jnp.exp2(s_s[at, h * qb : (h + 1) * qb] - peaks[h])
                s_s[at, h * qb : (h + 1) * qb] = e
                out.append(totals[h] + fold(e, jnp.sum))
            return tuple(out)

        totals = lax.fori_loop(
            lo, block + 1, expo, tuple(jnp.zeros((8, qb), F32) for _ in range(heads))
        )
        inverse = [1.0 / jnp.sum(t, axis=0, keepdims=True) for t in totals]

        def gather(kb, carry):
            at = pl.ds(pl.multiple_of(kb * qb, qb), qb)
            for h in range(heads):
                part = c_s[h, at, :]
                for v in range(qb // 128):
                    e = s_s[at, h * qb + v * 128 : h * qb + (v + 1) * 128]
                    part = part + e * inverse[h][:, v * 128 : (v + 1) * 128]
                c_s[h, at, :] = part
            return carry

        lax.fori_loop(lo, block + 1, gather, 0)

    @pl.when(i == last)
    def _():
        member = members(0, rows)
        parts = []
        for h in range(heads):
            mass = jnp.sum(c_s[h], axis=-1, keepdims=True)
            mixed = mass * v_s[...].astype(F32)
            high = mixed.astype(BF16)
            low = (mixed - high.astype(F32)).astype(BF16)
            parts.append(
                jnp.dot(member, high, preferred_element_type=F32)
                + jnp.dot(member, low, preferred_element_type=F32)
            )
        attended = jnp.concatenate(parts, axis=-1)
        high = attended.astype(BF16)
        low = (attended - high.astype(F32)).astype(BF16)
        wo_copy.wait()
        for p in range(n_mp):
            w = wo_s[:, p * share : (p + 1) * share]
            hp_ref[p] = jnp.dot(high, w, preferred_element_type=F32) + jnp.dot(
                low, w, preferred_element_type=F32
            )


def score_kernel(
    dims, hp_ref, ts_ref, ln_ref, ep_ref, cl_ref, fl_ref, lp_ref, pr_ref,
    rs_buf, ag_buf, g_buf, d_buf, rs_send, rs_recv, ag_send, ag_recv, g_send, g_recv,
):
    n_dp, n_mp, slots, share, width, nseq, classes = dims
    dp = lax.axis_index("dp")
    mp = lax.axis_index("mp")
    barrier = pltpu.get_barrier_semaphore()
    for d in range(1, n_mp):
        pl.semaphore_signal(barrier, inc=1, device_id=(dp, lax.rem(mp + d, n_mp)), device_id_type=MESH)
    for d in range(1, n_dp):
        pl.semaphore_signal(barrier, inc=1, device_id=(lax.rem(dp + d, n_dp), mp), device_id_type=MESH)
    pl.semaphore_wait(barrier, n_mp + n_dp - 2)

    rs = []
    for d in range(1, n_mp):
        peer = lax.rem(mp + d, n_mp)
        rs.append(pltpu.make_async_remote_copy(
            src_ref=hp_ref.at[peer], dst_ref=rs_buf.at[d - 1], send_sem=rs_send.at[d - 1],
            recv_sem=rs_recv.at[d - 1], device_id=(dp, peer), device_id_type=MESH,
        ))
        rs[-1].start()
    pooled = ts_ref[...] + hp_ref[mp]
    slot = lax.broadcasted_iota(jnp.int32, (slots, share), 0)
    count = jnp.ones((slots, share), F32)
    for j in range(slots):
        count = jnp.where(slot == j, ln_ref[j].astype(F32), count)
    for d in range(1, n_mp):
        rs[d - 1].wait_recv()
        pooled = pooled + rs_buf[d - 1]
    own = pl.ds(pl.multiple_of(dp * slots, slots), slots)
    ag_buf[own, :] = pooled / count

    ag = []
    for d in range(1, n_dp):
        peer = lax.rem(dp + d, n_dp)
        ag.append(pltpu.make_async_remote_copy(
            src_ref=ag_buf.at[own, :], dst_ref=ag_buf.at[own, :], send_sem=ag_send.at[d - 1],
            recv_sem=ag_recv.at[d - 1], device_id=(peer, mp), device_id_type=MESH,
        ))
        ag[-1].start()
    for d in range(1, n_mp):
        rs[d - 1].wait_send()
    for d in range(1, n_dp):
        ag[d - 1].wait_recv()

    every = ag_buf[...]
    g_buf[mp] = lax.dot_general(
        every, every, (((1,), (1,)), ((), ())), precision=HIGHEST, preferred_element_type=F32
    )
    gs = []
    for d in range(1, n_mp):
        peer = lax.rem(mp + d, n_mp)
        gs.append(pltpu.make_async_remote_copy(
            src_ref=g_buf.at[mp], dst_ref=g_buf.at[mp], send_sem=g_send.at[d - 1],
            recv_sem=g_recv.at[d - 1], device_id=(dp, peer), device_id_type=MESH,
        ))
        gs[-1].start()
    for d in range(1, n_dp):
        ag[d - 1].wait_send()

    label = ep_ref[...] * WAYS + cl_ref[...]
    support = fl_ref[...] == 0
    class_row = lax.broadcasted_iota(jnp.int32, (classes, nseq), 0)
    select = jnp.where((class_row == label) & support, 1.0, 0.0)
    a = lax.broadcasted_iota(jnp.int32, (slots, nseq), 0) + dp * slots
    mine = a == lax.broadcasted_iota(jnp.int32, (slots, nseq), 1)
    own_query = jnp.sum(jnp.where(mine, fl_ref[...].astype(F32), 0.0), axis=-1, keepdims=True)
    own_episode = jnp.sum(jnp.where(mine, ep_ref[...].astype(F32), 0.0), axis=-1, keepdims=True)

    for d in range(1, n_mp):
        gs[d - 1].wait_recv()
    gram = g_buf[0]
    for p in range(1, n_mp):
        gram = gram + g_buf[p]
    eye = lax.broadcasted_iota(jnp.int32, (nseq, nseq), 0) == lax.broadcasted_iota(
        jnp.int32, (nseq, nseq), 1
    )
    diag = jnp.where(eye, gram, 0.0)
    scale_row = lax.rsqrt(jnp.sum(diag, axis=0, keepdims=True) / width + 1e-06)
    scale_col = lax.rsqrt(jnp.sum(diag, axis=1, keepdims=True) / width + 1e-06)
    gram = gram * scale_row * scale_col
    cross_t = jnp.dot(select, gram, precision=HIGHEST, preferred_element_type=F32)
    norm_col = jnp.maximum(jnp.sum(cross_t * select, axis=1, keepdims=True), 0.0)
    proto_col = lax.rsqrt(norm_col / width + 1e-06)
    sums = jnp.dot(select * scale_row, every, precision=HIGHEST, preferred_element_type=F32)
    pr_ref[...] = sums * proto_col

    d_buf[...] = gram
    mine_gram = d_buf[own, :]
    cross = lax.dot_general(
        mine_gram, select, (((1,), (1,)), ((), ())), precision=HIGHEST, preferred_element_type=F32
    )
    eye_c = lax.broadcasted_iota(jnp.int32, (classes, classes), 0) == lax.broadcasted_iota(
        jnp.int32, (classes, classes), 1
    )
    norm_row = jnp.sum(jnp.where(eye_c, norm_col, 0.0), axis=0, keepdims=True)
    proto_row = lax.rsqrt(norm_row / width + 1e-06)
    own_norm = jnp.sum(jnp.where(mine, mine_gram, 0.0), axis=-1, keepdims=True)
    distance = own_norm - 2.0 * (cross * proto_row) + norm_row * proto_row * proto_row
    picked = jnp.zeros((slots, WAYS), F32)
    for e in range(classes // WAYS):
        picked = jnp.where(own_episode == float(e), distance[:, e * WAYS : (e + 1) * WAYS], picked)
    logits = -picked / math.sqrt(width)
    shifted = logits - jnp.max(logits, axis=-1, keepdims=True)
    logp = shifted - jnp.log(jnp.sum(jnp.exp(shifted), axis=-1, keepdims=True))
    lp_ref[...] = jnp.where(own_query == 1.0, logp, 0.0)
    for d in range(1, n_mp):
        gs[d - 1].wait_send()


def per_device(
    n_dp, n_mp, tokens, norm_gain, w_query, w_key, w_value, w_out,
    seq_starts, seq_lengths, episode_ids, class_ids, query_flags,
):
    rows, width = tokens.shape
    slots = seq_starts.shape[0]
    hd = HEAD_DIM
    heads = w_query.shape[1] // hd
    assert w_key.shape[1] == hd
    share = width // n_mp
    tile = pick(rows, (512, 256, 128))
    qb = pick(tile, (256, 128))
    chunk = pick(width, (512, 256, 128))
    frequency = ROPE_BASE ** (-np.arange(hd // 2, dtype=np.float64) * 2.0 / hd)
    angles = np.arange(rows, dtype=np.float64)[:, None] * frequency[None, :]
    cos = jnp.asarray(np.concatenate([np.cos(angles)] * 2, axis=1), F32)
    sin = jnp.asarray(np.concatenate([-np.sin(angles), np.sin(angles)], axis=1), F32)
    smem = pl.BlockSpec(memory_space=pltpu.SMEM)
    vmem = pl.BlockSpec(memory_space=pltpu.VMEM)
    hbm = pl.BlockSpec(memory_space=pl.ANY)
    dims = (rows, tile, qb, width, slots, heads, chunk, share, n_mp)
    head_part, token_sums = pl.pallas_call(
        functools.partial(encode_kernel, dims),
        grid=(rows // tile,),
        out_shape=(
            jax.ShapeDtypeStruct((n_mp, slots, share), F32),
            jax.ShapeDtypeStruct((slots, share), F32),
        ),
        in_specs=[
            smem, smem,
            pl.BlockSpec((tile, width), lambda i: (i, 0)),
            pl.BlockSpec((1, width), lambda i: (0, 0)),
            hbm, hbm, hbm, hbm,
            pl.BlockSpec((tile, hd), lambda i: (i, 0)),
            pl.BlockSpec((tile, hd), lambda i: (i, 0)),
        ],
        out_specs=(
            pl.BlockSpec((n_mp, slots, share), lambda i: (0, 0, 0)),
            pl.BlockSpec((slots, share), lambda i: (0, 0)),
        ),
        scratch_shapes=[
            pltpu.VMEM((width, (heads + 2) * hd), BF16),
            pltpu.VMEM(w_out.shape, BF16),
            pltpu.VMEM((heads, tile, hd), BF16),
            pltpu.VMEM((rows, hd), BF16),
            pltpu.VMEM((rows, hd), BF16),
            pltpu.VMEM((rows, heads * qb), F32),
            pltpu.VMEM((heads, rows, hd), F32),
            pltpu.SemaphoreType.DMA((width // chunk, 3)),
            pltpu.SemaphoreType.DMA,
        ],
        compiler_params=pltpu.CompilerParams(
            dimension_semantics=("arbitrary",), vmem_limit_bytes=60 * 1024 * 1024
        ),
    )(
        seq_starts, seq_lengths, tokens, norm_gain.reshape(1, width),
        w_query, w_key, w_value, w_out, cos, sin,
    )
    nseq = episode_ids.shape[0]
    episodes = max(1, nseq // (2 * WAYS))
    classes = episodes * WAYS
    dims = (n_dp, n_mp, slots, share, width, nseq, classes)
    dma = pltpu.SemaphoreType.DMA
    return pl.pallas_call(
        functools.partial(score_kernel, dims),
        out_shape=(
            jax.ShapeDtypeStruct((slots, WAYS), F32),
            jax.ShapeDtypeStruct((classes, share), F32),
        ),
        in_specs=[vmem, vmem, smem, vmem, vmem, vmem],
        out_specs=(vmem, vmem),
        scratch_shapes=[
            pltpu.VMEM((n_mp - 1, slots, share), F32),
            pltpu.VMEM((nseq, share), F32),
            pltpu.VMEM((n_mp, nseq, nseq), F32),
            pltpu.VMEM((nseq, nseq), F32),
            dma((n_mp - 1,)), dma((n_mp - 1,)),
            dma((n_dp - 1,)), dma((n_dp - 1,)),
            dma((n_mp - 1,)), dma((n_mp - 1,)),
        ],
        compiler_params=pltpu.CompilerParams(collective_id=0, has_side_effects=True),
    )(
        head_part, token_sums, seq_lengths,
        episode_ids.reshape(1, nseq), class_ids.reshape(1, nseq), query_flags.reshape(1, nseq),
    )


def solution(mesh):
    placed = (
        P("dp", None), P(), P(None, "mp"), P(None, "mp"), P(None, "mp"), P("mp", None),
        P("dp"), P("dp"), P(), P(), P(),
    )
    return jax.shard_map(
        functools.partial(per_device, mesh.shape["dp"], mesh.shape["mp"]),
        mesh=mesh,
        in_specs=placed,
        out_specs=(P("dp", None), P(None, "mp")),
        check_vma=False,
    )
```

```python
import functools
import math

import numpy as np
import jax
import jax.numpy as jnp
from jax import lax
from jax.experimental import pallas as pl
from jax.experimental.pallas import tpu as pltpu
from jax.sharding import PartitionSpec as P

HEAD_DIM = 128
WAYS = 32
ROPE_BASE = 500000.0
NEG_FILL = -1e30
MESH = pl.DeviceIdType.MESH
F32 = jnp.float32
BF16 = jnp.bfloat16
HIGHEST = lax.Precision.HIGHEST


def pick(total, options):
    for candidate in options:
        if total % candidate == 0:
            return candidate
    return total


def encode_kernel(
    dims, st_ref, ln_ref, x_hbm, gain_ref, wq_hbm, wk_hbm, wv_hbm, wo_hbm, cos_ref, sin_ref,
    hp_ref, ts_ref, x_s, acc_s, sq_s, w_s, wo_s, q_s, k_s, v_s, s_s, c_s, w_sem, wo_sem, x0_sem, x_sem,
):
    rows, tile, qb, width, slots, heads, chunk, share, n_mp = dims
    hd = HEAD_DIM
    i = pl.program_id(0)
    last = pl.num_programs(0) - 1
    q_cols = heads * hd
    chunks = width // chunk
    rank = lax.axis_index("mp")
    wo_copy = pltpu.make_async_copy(wo_hbm, wo_s, wo_sem)
    now = lax.rem(i, 2)
    x_ref = x_s.at[now]

    def fetch(t, slot):
        r = pl.ds(pl.multiple_of(t * tile, tile), tile)
        return pltpu.make_async_copy(x_hbm.at[r, :], x_s.at[slot], x_sem.at[slot])

    def squares(at, count, add):
        half = tile // 2
        for b in range(2):
            r = slice(b * half, (b + 1) * half)
            acc = sq_s[r, :] if add else jnp.zeros((half, 128), F32)
            for v in range(at, at + count, 128):
                x = x_ref[r, v : v + 128].astype(F32)
                acc = acc + x * x
            sq_s[r, :] = acc

    def members(first, count):
        slot = lax.broadcasted_iota(jnp.int32, (slots, count), 0)
        token = lax.broadcasted_iota(jnp.int32, (slots, count), 1) + first
        lo = jnp.zeros((slots, count), jnp.int32)
        hi = jnp.zeros((slots, count), jnp.int32)
        for j in range(slots):
            lo = jnp.where(slot == j, st_ref[j], lo)
            hi = jnp.where(slot == j, st_ref[j] + ln_ref[j], hi)
        return jnp.where((token >= lo) & (token < hi), 1.0, 0.0).astype(BF16)

    @pl.when(i == 0)
    def _():
        def copies(c):
            r = pl.ds(c * chunk, chunk)
            return (
                pltpu.make_async_copy(x_hbm.at[pl.ds(0, tile), r], x_s.at[0, :, r], x0_sem.at[c]),
                pltpu.make_async_copy(wq_hbm.at[r, :], w_s.at[r, pl.ds(0, q_cols)], w_sem.at[c, 0]),
                pltpu.make_async_copy(wk_hbm.at[r, :], w_s.at[r, pl.ds(q_cols, hd)], w_sem.at[c, 1]),
                pltpu.make_async_copy(wv_hbm.at[r, :], w_s.at[r, pl.ds(q_cols + hd, hd)], w_sem.at[c, 2]),
            )

        for c in range(chunks):
            for copy in copies(c):
                copy.start()
        if rows > tile:
            fetch(1, 1).start()
        wo_copy.start()
        ts_ref[...] = jnp.zeros_like(ts_ref)
        c_s[...] = jnp.zeros_like(c_s)
        for c in range(chunks):
            for copy in copies(c):
                copy.wait()
            for b in range(chunk // 128):
                at = c * chunk + b * 128
                g = jnp.broadcast_to(gain_ref[at : at + 128].astype(F32)[None, :], (128, 128)).T
                for v in range(heads + 2):
                    w = w_s[at : at + 128, v * hd : (v + 1) * hd].astype(F32)
                    w_s[at : at + 128, v * hd : (v + 1) * hd] = (w * g).astype(BF16)
            r = slice(c * chunk, (c + 1) * chunk)
            part = jnp.dot(x_s[0, :, r], w_s[r, :], preferred_element_type=F32)
            acc_s[...] = part if c == 0 else acc_s[...] + part
            squares(c * chunk, chunk, c > 0)

    @pl.when(i > 0)
    def _():
        fetch(i, now).wait()

        @pl.when(i < last)
        def _():
            fetch(i + 1, 1 - now).start()

        acc_s[...] = jnp.dot(x_ref[...], w_s[...], preferred_element_type=F32)
        squares(0, width, False)

    rstd = lax.rsqrt(jnp.sum(sq_s[...], axis=-1, keepdims=True) / width + 1e-05)
    proj = acc_s
    cos = cos_ref[...]
    sin = sin_ref[...]

    def rope(y):
        return (y * cos + pltpu.roll(y, hd // 2, 1) * sin).astype(BF16)

    q_rstd = rstd * (math.log2(math.e) / math.sqrt(hd))
    for h in range(heads):
        q_s[h] = rope(proj[:, h * hd : (h + 1) * hd] * q_rstd)
    here = pl.ds(pl.multiple_of(i * tile, tile), tile)
    k_s[here, :] = rope(proj[:, q_cols : q_cols + hd] * rstd)
    v_s[here, :] = (proj[:, q_cols + hd : q_cols + 2 * hd] * rstd).astype(BF16)
    cols = pl.ds(pl.multiple_of(rank * share, share), share)
    ts_ref[...] += jnp.dot(members(i * tile, tile), x_ref[:, cols], preferred_element_type=F32)

    for b in range(tile // qb):
        block = i * (tile // qb) + b
        first = block * qb
        lo_row = first
        token = lax.broadcasted_iota(jnp.int32, (1, qb), 1) + first
        start = token
        for j in range(slots):
            s0 = st_ref[j]
            s1 = s0 + ln_ref[j]
            start = jnp.where((token >= s0) & (token < s1), s0, start)
            lo_row = jnp.where((first >= s0) & (first < s1), s0, lo_row)
        lo = lo_row // qb

        def fold(a, op):
            return op(a.reshape(qb // 8, 8, qb), axis=0)

        def score(kb, peaks):
            at = pl.ds(pl.multiple_of(kb * qb, qb), qb)
            keys = k_s[at, :]
            row = lax.broadcasted_iota(jnp.int32, (qb, qb), 0) + kb * qb
            ok = (row >= start) & (row <= token)
            out = []
            for h in range(heads):
                s = lax.dot_general(
                    keys, q_s[h, b * qb : (b + 1) * qb, :], (((1,), (1,)), ((), ())),
                    preferred_element_type=F32,
                )
                s = jnp.where(ok, s, NEG_FILL)
                s_s[at, h * qb : (h + 1) * qb] = s
                out.append(jnp.maximum(peaks[h], fold(s, jnp.max)))
            return tuple(out)

        peaks = lax.fori_loop(
            lo, block + 1, score, tuple(jnp.full((8, qb), NEG_FILL, F32) for _ in range(heads))
        )
        peaks = [jnp.max(p, axis=0, keepdims=True) for p in peaks]

        def expo(kb, totals):
            at = pl.ds(pl.multiple_of(kb * qb, qb), qb)
            out = []
            for h in range(heads):
                e = jnp.exp2(s_s[at, h * qb : (h + 1) * qb] - peaks[h])
                s_s[at, h * qb : (h + 1) * qb] = e
                out.append(totals[h] + fold(e, jnp.sum))
            return tuple(out)

        totals = lax.fori_loop(
            lo, block + 1, expo, tuple(jnp.zeros((8, qb), F32) for _ in range(heads))
        )
        inverse = [1.0 / jnp.sum(t, axis=0, keepdims=True) for t in totals]

        def gather(kb, carry):
            at = pl.ds(pl.multiple_of(kb * qb, qb), qb)
            for h in range(heads):
                part = c_s[h, at, :]
                for v in range(qb // 128):
                    e = s_s[at, h * qb + v * 128 : h * qb + (v + 1) * 128]
                    part = part + e * inverse[h][:, v * 128 : (v + 1) * 128]
                c_s[h, at, :] = part
            return carry

        lax.fori_loop(lo, block + 1, gather, 0)

    @pl.when(i == last)
    def _():
        member = members(0, rows)
        parts = []
        for h in range(heads):
            mass = jnp.sum(c_s[h], axis=-1, keepdims=True)
            mixed = mass * v_s[...].astype(F32)
            parts.append(jnp.dot(member, mixed.astype(BF16), preferred_element_type=F32))
        attended = jnp.concatenate(parts, axis=-1)
        high = attended.astype(BF16)
        low = attended - high.astype(F32)
        both = jnp.concatenate([high.astype(F32), low], axis=0).astype(BF16)
        wo_copy.wait()
        for p in range(n_mp):
            w = wo_s[:, p * share : (p + 1) * share]
            out = jnp.dot(both, w, preferred_element_type=F32)
            hp_ref[p] = out[:slots] + out[slots:]


def exchange_kernel(
    dims, hp_ref, ts_ref, ln_ref, every_ref, gram_ref,
    rs_buf, ag_buf, g_buf, rs_send, rs_recv, ag_send, ag_recv, g_send, g_recv,
):
    n_dp, n_mp, slots, share, nseq, pieces, fold = dims
    dp = lax.axis_index("dp")
    mp = lax.axis_index("mp")
    barrier = pltpu.get_barrier_semaphore()
    for d in range(1, n_mp):
        pl.semaphore_signal(barrier, inc=1, device_id=(dp, lax.rem(mp + d, n_mp)), device_id_type=MESH)
    for d in range(1, n_dp):
        pl.semaphore_signal(barrier, inc=1, device_id=(lax.rem(dp + d, n_dp), mp), device_id_type=MESH)
    pl.semaphore_wait(barrier, n_mp + n_dp - 2)

    piece = share // pieces
    rs = {}
    for c in range(pieces):
        cols = pl.ds(c * piece, piece)
        for d in range(1, n_mp):
            peer = lax.rem(mp + d, n_mp)
            rs[c, d] = pltpu.make_async_remote_copy(
                src_ref=hp_ref.at[peer, :, cols], dst_ref=rs_buf.at[d - 1, c],
                send_sem=rs_send.at[c, d - 1], recv_sem=rs_recv.at[c, d - 1],
                device_id=(dp, peer), device_id_type=MESH,
            )
            rs[c, d].start()
    slot = lax.broadcasted_iota(jnp.int32, (slots, piece), 0)
    count = jnp.ones((slots, piece), F32)
    for j in range(slots):
        count = jnp.where(slot == j, ln_ref[j].astype(F32), count)
    own = pl.ds(pl.multiple_of(dp * slots, slots), slots)
    ag = {}
    for c in range(pieces):
        cols = slice(c * piece, (c + 1) * piece)
        pooled = ts_ref[:, cols] + hp_ref[mp, :, cols]
        for d in range(1, n_mp):
            rs[c, d].wait_recv()
            pooled = pooled + rs_buf[d - 1, c]
        ag_buf[c, own, :] = pooled / count
        for d in range(1, n_dp):
            peer = lax.rem(dp + d, n_dp)
            ag[c, d] = pltpu.make_async_remote_copy(
                src_ref=ag_buf.at[c, own, :], dst_ref=ag_buf.at[c, own, :],
                send_sem=ag_send.at[c, d - 1], recv_sem=ag_recv.at[c, d - 1],
                device_id=(peer, mp), device_id_type=MESH,
            )
            ag[c, d].start()
    part = None
    for c in range(pieces):
        for d in range(1, n_dp):
            ag[c, d].wait_recv()
        block = ag_buf[c]
        every_ref[:, c * piece : (c + 1) * piece] = block
        term = lax.dot_general(
            block, block, (((1,), (1,)), ((), ())), precision=HIGHEST, preferred_element_type=F32
        )
        part = term if part is None else part + term
    tall = nseq // fold
    g_buf[mp] = jnp.concatenate([part[f * tall : (f + 1) * tall] for f in range(fold)], axis=1)
    gs = {}
    for d in range(1, n_mp):
        peer = lax.rem(mp + d, n_mp)
        gs[d] = pltpu.make_async_remote_copy(
            src_ref=g_buf.at[mp], dst_ref=g_buf.at[mp], send_sem=g_send.at[d - 1],
            recv_sem=g_recv.at[d - 1], device_id=(dp, peer), device_id_type=MESH,
        )
        gs[d].start()
    for copy in list(rs.values()) + list(ag.values()):
        copy.wait_send()
    for d in range(1, n_mp):
        gs[d].wait_recv()
    gram = g_buf[0]
    for p in range(1, n_mp):
        gram = gram + g_buf[p]
    gram_ref[...] = jnp.concatenate(
        [gram[:, f * nseq : (f + 1) * nseq] for f in range(fold)], axis=0
    )
    for d in range(1, n_mp):
        gs[d].wait_send()


def score_kernel(dims, every_ref, gram_ref, ep_ref, cl_ref, fl_ref, lp_ref, pr_ref, d_buf):
    slots, width, nseq, classes = dims
    dp = lax.axis_index("dp")
    own = pl.ds(pl.multiple_of(dp * slots, slots), slots)
    every = every_ref[...]
    gram = gram_ref[...]
    label = ep_ref[...] * WAYS + cl_ref[...]
    support = fl_ref[...] == 0
    class_row = lax.broadcasted_iota(jnp.int32, (classes, nseq), 0)
    select = jnp.where((class_row == label) & support, 1.0, 0.0)
    a = lax.broadcasted_iota(jnp.int32, (slots, nseq), 0) + dp * slots
    mine = a == lax.broadcasted_iota(jnp.int32, (slots, nseq), 1)
    own_query = jnp.sum(jnp.where(mine, fl_ref[...].astype(F32), 0.0), axis=-1, keepdims=True)
    own_episode = jnp.sum(jnp.where(mine, ep_ref[...].astype(F32), 0.0), axis=-1, keepdims=True)
    eye = lax.broadcasted_iota(jnp.int32, (nseq, nseq), 0) == lax.broadcasted_iota(
        jnp.int32, (nseq, nseq), 1
    )
    diag = jnp.where(eye, gram, 0.0)
    scale_row = lax.rsqrt(jnp.sum(diag, axis=0, keepdims=True) / width + 1e-06)
    scale_col = lax.rsqrt(jnp.sum(diag, axis=1, keepdims=True) / width + 1e-06)
    gram = gram * scale_row * scale_col
    cross_t = jnp.dot(select, gram, precision=HIGHEST, preferred_element_type=F32)
    norm_col = jnp.maximum(jnp.sum(cross_t * select, axis=1, keepdims=True), 0.0)
    proto_col = lax.rsqrt(norm_col / width + 1e-06)
    sums = jnp.dot(select * scale_row, every, precision=HIGHEST, preferred_element_type=F32)
    pr_ref[...] = sums * proto_col

    d_buf[...] = gram
    mine_gram = d_buf[own, :]
    cross = lax.dot_general(
        mine_gram, select, (((1,), (1,)), ((), ())), precision=HIGHEST, preferred_element_type=F32
    )
    eye_c = lax.broadcasted_iota(jnp.int32, (classes, classes), 0) == lax.broadcasted_iota(
        jnp.int32, (classes, classes), 1
    )
    norm_row = jnp.sum(jnp.where(eye_c, norm_col, 0.0), axis=0, keepdims=True)
    proto_row = lax.rsqrt(norm_row / width + 1e-06)
    own_norm = jnp.sum(jnp.where(mine, mine_gram, 0.0), axis=-1, keepdims=True)
    distance = own_norm - 2.0 * (cross * proto_row) + norm_row * proto_row * proto_row
    picked = jnp.zeros((slots, WAYS), F32)
    for e in range(classes // WAYS):
        picked = jnp.where(own_episode == float(e), distance[:, e * WAYS : (e + 1) * WAYS], picked)
    logits = -picked / math.sqrt(width)
    shifted = logits - jnp.max(logits, axis=-1, keepdims=True)
    logp = shifted - jnp.log(jnp.sum(jnp.exp(shifted), axis=-1, keepdims=True))
    lp_ref[...] = jnp.where(own_query == 1.0, logp, 0.0)


def per_device(
    n_dp, n_mp, tokens, norm_gain, w_query, w_key, w_value, w_out,
    seq_starts, seq_lengths, episode_ids, class_ids, query_flags,
):
    rows, width = tokens.shape
    slots = seq_starts.shape[0]
    hd = HEAD_DIM
    heads = w_query.shape[1] // hd
    assert w_key.shape[1] == hd
    share = width // n_mp
    tile = pick(rows, (512, 256, 128))
    qb = pick(tile, (256, 128))
    chunk = pick(width, (512, 256, 128))
    frequency = ROPE_BASE ** (-np.arange(hd // 2, dtype=np.float64) * 2.0 / hd)
    angles = np.arange(rows, dtype=np.float64)[:, None] * frequency[None, :]
    cos = jnp.asarray(np.concatenate([np.cos(angles)] * 2, axis=1), F32)
    sin = jnp.asarray(np.concatenate([-np.sin(angles), np.sin(angles)], axis=1), F32)
    smem = pl.BlockSpec(memory_space=pltpu.SMEM)
    vmem = pl.BlockSpec(memory_space=pltpu.VMEM)
    hbm = pl.BlockSpec(memory_space=pl.ANY)
    dims = (rows, tile, qb, width, slots, heads, chunk, share, n_mp)
    head_part, token_sums = pl.pallas_call(
        functools.partial(encode_kernel, dims),
        grid=(rows // tile,),
        out_shape=(
            jax.ShapeDtypeStruct((n_mp, slots, share), F32),
            jax.ShapeDtypeStruct((slots, share), F32),
        ),
        in_specs=[
            smem, smem,
            hbm,
            vmem,
            hbm, hbm, hbm, hbm,
            pl.BlockSpec((tile, hd), lambda i: (i, 0)),
            pl.BlockSpec((tile, hd), lambda i: (i, 0)),
        ],
        out_specs=(
            pl.BlockSpec((n_mp, slots, share), lambda i: (0, 0, 0)),
            pl.BlockSpec((slots, share), lambda i: (0, 0)),
        ),
        scratch_shapes=[
            pltpu.VMEM((2, tile, width), BF16),
            pltpu.VMEM((tile, (heads + 2) * hd), F32),
            pltpu.VMEM((tile, 128), F32),
            pltpu.VMEM((width, (heads + 2) * hd), BF16),
            pltpu.VMEM(w_out.shape, BF16),
            pltpu.VMEM((heads, tile, hd), BF16),
            pltpu.VMEM((rows, hd), BF16),
            pltpu.VMEM((rows, hd), BF16),
            pltpu.VMEM((rows, heads * qb), F32),
            pltpu.VMEM((heads, rows, hd), F32),
            pltpu.SemaphoreType.DMA((width // chunk, 3)),
            pltpu.SemaphoreType.DMA,
            pltpu.SemaphoreType.DMA((width // chunk,)),
            pltpu.SemaphoreType.DMA((2,)),
        ],
        compiler_params=pltpu.CompilerParams(
            dimension_semantics=("arbitrary",), vmem_limit_bytes=60 * 1024 * 1024
        ),
    )(
        seq_starts, seq_lengths, tokens, norm_gain,
        w_query, w_key, w_value, w_out, cos, sin,
    )
    nseq = episode_ids.shape[0]
    episodes = max(1, nseq // (2 * WAYS))
    classes = episodes * WAYS
    dma = pltpu.SemaphoreType.DMA
    pieces = 2 if share % 256 == 0 else 1
    fold = 2 if nseq <= 64 else 1
    dims = (n_dp, n_mp, slots, share, nseq, pieces, fold)
    every, gram = pl.pallas_call(
        functools.partial(exchange_kernel, dims),
        out_shape=(
            jax.ShapeDtypeStruct((nseq, share), F32),
            jax.ShapeDtypeStruct((nseq, nseq), F32),
        ),
        in_specs=[vmem, vmem, smem],
        out_specs=(vmem, vmem),
        scratch_shapes=[
            pltpu.VMEM((n_mp - 1, pieces, slots, share // pieces), F32),
            pltpu.VMEM((pieces, nseq, share // pieces), F32),
            pltpu.VMEM((n_mp, nseq // fold, nseq * fold), F32),
            dma((pieces, n_mp - 1)), dma((pieces, n_mp - 1)),
            dma((pieces, n_dp - 1)), dma((pieces, n_dp - 1)),
            dma((n_mp - 1,)), dma((n_mp - 1,)),
        ],
        compiler_params=pltpu.CompilerParams(collective_id=0, has_side_effects=True),
    )(head_part, token_sums, seq_lengths)
    return pl.pallas_call(
        functools.partial(score_kernel, (slots, width, nseq, classes)),
        out_shape=(
            jax.ShapeDtypeStruct((slots, WAYS), F32),
            jax.ShapeDtypeStruct((classes, share), F32),
        ),
        in_specs=[vmem] * 5,
        out_specs=(vmem, vmem),
        scratch_shapes=[pltpu.VMEM((nseq, nseq), F32)],
    )(
        every, gram,
        episode_ids.reshape(1, nseq), class_ids.reshape(1, nseq), query_flags.reshape(1, nseq),
    )


def solution(mesh):
    placed = (
        P("dp", None), P(), P(None, "mp"), P(None, "mp"), P(None, "mp"), P("mp", None),
        P("dp"), P("dp"), P(), P(), P(),
    )
    return jax.shard_map(
        functools.partial(per_device, mesh.shape["dp"], mesh.shape["mp"]),
        mesh=mesh,
        in_specs=placed,
        out_specs=(P("dp", None), P(None, "mp")),
        check_vma=False,
    )
```

```python
import functools
import math

import numpy as np
import jax
import jax.numpy as jnp
from jax import lax
from jax.experimental import pallas as pl
from jax.experimental.pallas import tpu as pltpu
from jax.sharding import PartitionSpec as P

HEAD_DIM = 128
WAYS = 32
ROPE_BASE = 500000.0
NEG_FILL = -1e30
MESH = pl.DeviceIdType.MESH
F32 = jnp.float32
BF16 = jnp.bfloat16
HIGHEST = lax.Precision.HIGHEST


def pick(total, options):
    for candidate in options:
        if total % candidate == 0:
            return candidate
    return total


def encode_kernel(
    dims, st_ref, ln_ref, x_ref, gain_ref, wq_hbm, wk_hbm, wv_hbm, wo_hbm, cos_ref, sin_ref,
    hp_ref, ts_ref, w_s, wo_s, q_s, k_s, v_s, s_s, c_s, w_sem, wo_sem,
):
    rows, tile, qb, width, slots, heads, chunk, share, n_mp = dims
    hd = HEAD_DIM
    i = pl.program_id(0)
    last = pl.num_programs(0) - 1
    q_cols = heads * hd
    chunks = width // chunk
    rank = lax.axis_index("mp")
    wo_copy = pltpu.make_async_copy(wo_hbm, wo_s, wo_sem)

    def members(first, count):
        slot = lax.broadcasted_iota(jnp.int32, (slots, count), 0)
        token = lax.broadcasted_iota(jnp.int32, (slots, count), 1) + first
        lo = jnp.zeros((slots, count), jnp.int32)
        hi = jnp.zeros((slots, count), jnp.int32)
        for j in range(slots):
            lo = jnp.where(slot == j, st_ref[j], lo)
            hi = jnp.where(slot == j, st_ref[j] + ln_ref[j], hi)
        return jnp.where((token >= lo) & (token < hi), 1.0, 0.0).astype(BF16)

    @pl.when(i == 0)
    def _():
        def copies(c):
            r = pl.ds(c * chunk, chunk)
            return (
                pltpu.make_async_copy(wq_hbm.at[r, :], w_s.at[r, pl.ds(0, q_cols)], w_sem.at[c, 0]),
                pltpu.make_async_copy(wk_hbm.at[r, :], w_s.at[r, pl.ds(q_cols, hd)], w_sem.at[c, 1]),
                pltpu.make_async_copy(wv_hbm.at[r, :], w_s.at[r, pl.ds(q_cols + hd, hd)], w_sem.at[c, 2]),
            )

        for c in range(chunks):
            for copy in copies(c):
                copy.start()
        wo_copy.start()
        ts_ref[...] = jnp.zeros_like(ts_ref)
        c_s[...] = jnp.zeros_like(c_s)
        for c in range(chunks):
            for copy in copies(c):
                copy.wait()
            for b in range(chunk // 128):
                at = c * chunk + b * 128
                g = jnp.broadcast_to(gain_ref[at : at + 128].astype(F32)[None, :], (128, 128)).T
                for v in range(heads + 2):
                    w = w_s[at : at + 128, v * hd : (v + 1) * hd].astype(F32)
                    w_s[at : at + 128, v * hd : (v + 1) * hd] = (w * g).astype(BF16)

    half = tile // 2
    sums = []
    for b in range(2):
        acc = jnp.zeros((half, 128), F32)
        for v in range(width // 128):
            x = x_ref[b * half : (b + 1) * half, v * 128 : (v + 1) * 128].astype(F32)
            acc = acc + x * x
        sums.append(jnp.sum(acc, axis=-1, keepdims=True))
    rstd = lax.rsqrt(jnp.concatenate(sums, axis=0) / width + 1e-05)
    proj = jnp.dot(x_ref[...], w_s[...], preferred_element_type=F32)
    cos = cos_ref[...]
    sin = sin_ref[...]

    def rope(y):
        return (y * cos + pltpu.roll(y, hd // 2, 1) * sin).astype(BF16)

    q_rstd = rstd * (math.log2(math.e) / math.sqrt(hd))
    for h in range(heads):
        q_s[h] = rope(proj[:, h * hd : (h + 1) * hd] * q_rstd)
    here = pl.ds(pl.multiple_of(i * tile, tile), tile)
    k_s[here, :] = rope(proj[:, q_cols : q_cols + hd] * rstd)
    v_s[here, :] = (proj[:, q_cols + hd :] * rstd).astype(BF16)
    cols = pl.ds(pl.multiple_of(rank * share, share), share)
    ts_ref[...] += jnp.dot(members(i * tile, tile), x_ref[:, cols], preferred_element_type=F32)

    for b in range(tile // qb):
        block = i * (tile // qb) + b
        first = block * qb
        lo_row = first
        token = lax.broadcasted_iota(jnp.int32, (1, qb), 1) + first
        start = token
        for j in range(slots):
            s0 = st_ref[j]
            s1 = s0 + ln_ref[j]
            start = jnp.where((token >= s0) & (token < s1), s0, start)
            lo_row = jnp.where((first >= s0) & (first < s1), s0, lo_row)
        lo = lo_row // qb

        def fold(a, op):
            return op(a.reshape(qb // 8, 8, qb), axis=0)

        def score(kb, peaks):
            at = pl.ds(pl.multiple_of(kb * qb, qb), qb)
            keys = k_s[at, :]
            row = lax.broadcasted_iota(jnp.int32, (qb, qb), 0) + kb * qb
            ok = (row >= start) & (row <= token)
            out = []
            for h in range(heads):
                s = lax.dot_general(
                    keys, q_s[h, b * qb : (b + 1) * qb, :], (((1,), (1,)), ((), ())),
                    preferred_element_type=F32,
                )
                s = jnp.where(ok, s, NEG_FILL)
                s_s[at, h * qb : (h + 1) * qb] = s
                out.append(jnp.maximum(peaks[h], fold(s, jnp.max)))
            return tuple(out)

        peaks = lax.fori_loop(
            lo, block + 1, score, tuple(jnp.full((8, qb), NEG_FILL, F32) for _ in range(heads))
        )
        peaks = [jnp.max(p, axis=0, keepdims=True) for p in peaks]

        def expo(kb, totals):
            at = pl.ds(pl.multiple_of(kb * qb, qb), qb)
            out = []
            for h in range(heads):
                e = jnp.exp2(s_s[at, h * qb : (h + 1) * qb] - peaks[h])
                s_s[at, h * qb : (h + 1) * qb] = e
                out.append(totals[h] + fold(e, jnp.sum))
            return tuple(out)

        totals = lax.fori_loop(
            lo, block + 1, expo, tuple(jnp.zeros((8, qb), F32) for _ in range(heads))
        )
        inverse = [1.0 / jnp.sum(t, axis=0, keepdims=True) for t in totals]

        def gather(kb, carry):
            at = pl.ds(pl.multiple_of(kb * qb, qb), qb)
            for h in range(heads):
                part = c_s[h, at, :]
                for v in range(qb // 128):
                    e = s_s[at, h * qb + v * 128 : h * qb + (v + 1) * 128]
                    part = part + e * inverse[h][:, v * 128 : (v + 1) * 128]
                c_s[h, at, :] = part
            return carry

        lax.fori_loop(lo, block + 1, gather, 0)

    @pl.when(i == last)
    def _():
        member = members(0, rows)
        parts = []
        for h in range(heads):
            mass = jnp.sum(c_s[h], axis=-1, keepdims=True)
            mixed = mass * v_s[...].astype(F32)
            high = mixed.astype(BF16)
            low = (mixed - high.astype(F32)).astype(BF16)
            parts.append(
                jnp.dot(member, high, preferred_element_type=F32)
                + jnp.dot(member, low, preferred_element_type=F32)
            )
        attended = jnp.concatenate(parts, axis=-1)
        high = attended.astype(BF16)
        low = attended - high.astype(F32)
        both = jnp.concatenate([high.astype(F32), low], axis=0).astype(BF16)
        wo_copy.wait()
        for p in range(n_mp):
            w = wo_s[:, p * share : (p + 1) * share]
            out = jnp.dot(both, w, preferred_element_type=F32)
            hp_ref[p] = out[:slots] + out[slots:]


def exchange_kernel(
    dims, hp_ref, ts_ref, ln_ref, every_ref, gram_ref,
    rs_buf, ag_buf, g_buf, rs_send, rs_recv, ag_send, ag_recv, g_send, g_recv,
):
    n_dp, n_mp, slots, share, nseq, pieces, fold = dims
    dp = lax.axis_index("dp")
    mp = lax.axis_index("mp")
    barrier = pltpu.get_barrier_semaphore()
    for d in range(1, n_mp):
        pl.semaphore_signal(barrier, inc=1, device_id=(dp, lax.rem(mp + d, n_mp)), device_id_type=MESH)
    for d in range(1, n_dp):
        pl.semaphore_signal(barrier, inc=1, device_id=(lax.rem(dp + d, n_dp), mp), device_id_type=MESH)
    pl.semaphore_wait(barrier, n_mp + n_dp - 2)

    piece = share // pieces
    rs = {}
    for c in range(pieces):
        cols = pl.ds(c * piece, piece)
        for d in range(1, n_mp):
            peer = lax.rem(mp + d, n_mp)
            rs[c, d] = pltpu.make_async_remote_copy(
                src_ref=hp_ref.at[peer, :, cols], dst_ref=rs_buf.at[d - 1, c],
                send_sem=rs_send.at[c, d - 1], recv_sem=rs_recv.at[c, d - 1],
                device_id=(dp, peer), device_id_type=MESH,
            )
            rs[c, d].start()
    slot = lax.broadcasted_iota(jnp.int32, (slots, piece), 0)
    count = jnp.ones((slots, piece), F32)
    for j in range(slots):
        count = jnp.where(slot == j, ln_ref[j].astype(F32), count)
    own = pl.ds(pl.multiple_of(dp * slots, slots), slots)
    ag = {}
    for c in range(pieces):
        cols = slice(c * piece, (c + 1) * piece)
        pooled = ts_ref[:, cols] + hp_ref[mp, :, cols]
        for d in range(1, n_mp):
            rs[c, d].wait_recv()
            pooled = pooled + rs_buf[d - 1, c]
        ag_buf[c, own, :] = pooled / count
        for d in range(1, n_dp):
            peer = lax.rem(dp + d, n_dp)
            ag[c, d] = pltpu.make_async_remote_copy(
                src_ref=ag_buf.at[c, own, :], dst_ref=ag_buf.at[c, own, :],
                send_sem=ag_send.at[c, d - 1], recv_sem=ag_recv.at[c, d - 1],
                device_id=(peer, mp), device_id_type=MESH,
            )
            ag[c, d].start()
    part = None
    for c in range(pieces):
        for d in range(1, n_dp):
            ag[c, d].wait_recv()
        block = ag_buf[c]
        every_ref[:, c * piece : (c + 1) * piece] = block
        term = lax.dot_general(
            block, block, (((1,), (1,)), ((), ())), precision=HIGHEST, preferred_element_type=F32
        )
        part = term if part is None else part + term
    tall = nseq // fold
    g_buf[mp] = jnp.concatenate([part[f * tall : (f + 1) * tall] for f in range(fold)], axis=1)
    gs = {}
    for d in range(1, n_mp):
        peer = lax.rem(mp + d, n_mp)
        gs[d] = pltpu.make_async_remote_copy(
            src_ref=g_buf.at[mp], dst_ref=g_buf.at[mp], send_sem=g_send.at[d - 1],
            recv_sem=g_recv.at[d - 1], device_id=(dp, peer), device_id_type=MESH,
        )
        gs[d].start()
    for copy in list(rs.values()) + list(ag.values()):
        copy.wait_send()
    for d in range(1, n_mp):
        gs[d].wait_recv()
    gram = g_buf[0]
    for p in range(1, n_mp):
        gram = gram + g_buf[p]
    gram_ref[...] = jnp.concatenate(
        [gram[:, f * nseq : (f + 1) * nseq] for f in range(fold)], axis=0
    )
    for d in range(1, n_mp):
        gs[d].wait_send()


def score_kernel(dims, every_ref, gram_ref, ep_ref, cl_ref, fl_ref, lp_ref, pr_ref, d_buf):
    slots, width, nseq, classes = dims
    dp = lax.axis_index("dp")
    own = pl.ds(pl.multiple_of(dp * slots, slots), slots)
    every = every_ref[...]
    gram = gram_ref[...]
    label = ep_ref[...] * WAYS + cl_ref[...]
    support = fl_ref[...] == 0
    class_row = lax.broadcasted_iota(jnp.int32, (classes, nseq), 0)
    select = jnp.where((class_row == label) & support, 1.0, 0.0)
    a = lax.broadcasted_iota(jnp.int32, (slots, nseq), 0) + dp * slots
    mine = a == lax.broadcasted_iota(jnp.int32, (slots, nseq), 1)
    own_query = jnp.sum(jnp.where(mine, fl_ref[...].astype(F32), 0.0), axis=-1, keepdims=True)
    own_episode = jnp.sum(jnp.where(mine, ep_ref[...].astype(F32), 0.0), axis=-1, keepdims=True)
    eye = lax.broadcasted_iota(jnp.int32, (nseq, nseq), 0) == lax.broadcasted_iota(
        jnp.int32, (nseq, nseq), 1
    )
    diag = jnp.where(eye, gram, 0.0)
    scale_row = lax.rsqrt(jnp.sum(diag, axis=0, keepdims=True) / width + 1e-06)
    scale_col = lax.rsqrt(jnp.sum(diag, axis=1, keepdims=True) / width + 1e-06)
    gram = gram * scale_row * scale_col
    cross_t = jnp.dot(select, gram, precision=HIGHEST, preferred_element_type=F32)
    norm_col = jnp.maximum(jnp.sum(cross_t * select, axis=1, keepdims=True), 0.0)
    proto_col = lax.rsqrt(norm_col / width + 1e-06)
    sums = jnp.dot(select * scale_row, every, precision=HIGHEST, preferred_element_type=F32)
    pr_ref[...] = sums * proto_col

    d_buf[...] = gram
    mine_gram = d_buf[own, :]
    cross = lax.dot_general(
        mine_gram, select, (((1,), (1,)), ((), ())), precision=HIGHEST, preferred_element_type=F32
    )
    eye_c = lax.broadcasted_iota(jnp.int32, (classes, classes), 0) == lax.broadcasted_iota(
        jnp.int32, (classes, classes), 1
    )
    norm_row = jnp.sum(jnp.where(eye_c, norm_col, 0.0), axis=0, keepdims=True)
    proto_row = lax.rsqrt(norm_row / width + 1e-06)
    own_norm = jnp.sum(jnp.where(mine, mine_gram, 0.0), axis=-1, keepdims=True)
    distance = own_norm - 2.0 * (cross * proto_row) + norm_row * proto_row * proto_row
    picked = jnp.zeros((slots, WAYS), F32)
    for e in range(classes // WAYS):
        picked = jnp.where(own_episode == float(e), distance[:, e * WAYS : (e + 1) * WAYS], picked)
    logits = -picked / math.sqrt(width)
    shifted = logits - jnp.max(logits, axis=-1, keepdims=True)
    logp = shifted - jnp.log(jnp.sum(jnp.exp(shifted), axis=-1, keepdims=True))
    lp_ref[...] = jnp.where(own_query == 1.0, logp, 0.0)


def per_device(
    n_dp, n_mp, tokens, norm_gain, w_query, w_key, w_value, w_out,
    seq_starts, seq_lengths, episode_ids, class_ids, query_flags,
):
    rows, width = tokens.shape
    slots = seq_starts.shape[0]
    hd = HEAD_DIM
    heads = w_query.shape[1] // hd
    assert w_key.shape[1] == hd
    share = width // n_mp
    tile = pick(rows, (512, 256, 128))
    qb = pick(tile, (256, 128))
    chunk = pick(width, (512, 256, 128))
    frequency = ROPE_BASE ** (-np.arange(hd // 2, dtype=np.float64) * 2.0 / hd)
    angles = np.arange(rows, dtype=np.float64)[:, None] * frequency[None, :]
    cos = jnp.asarray(np.concatenate([np.cos(angles)] * 2, axis=1), F32)
    sin = jnp.asarray(np.concatenate([-np.sin(angles), np.sin(angles)], axis=1), F32)
    smem = pl.BlockSpec(memory_space=pltpu.SMEM)
    vmem = pl.BlockSpec(memory_space=pltpu.VMEM)
    hbm = pl.BlockSpec(memory_space=pl.ANY)
    dims = (rows, tile, qb, width, slots, heads, chunk, share, n_mp)
    head_part, token_sums = pl.pallas_call(
        functools.partial(encode_kernel, dims),
        grid=(rows // tile,),
        out_shape=(
            jax.ShapeDtypeStruct((n_mp, slots, share), F32),
            jax.ShapeDtypeStruct((slots, share), F32),
        ),
        in_specs=[
            smem, smem,
            pl.BlockSpec((tile, width), lambda i: (i, 0)),
            vmem,
            hbm, hbm, hbm, hbm,
            pl.BlockSpec((tile, hd), lambda i: (i, 0)),
            pl.BlockSpec((tile, hd), lambda i: (i, 0)),
        ],
        out_specs=(
            pl.BlockSpec((n_mp, slots, share), lambda i: (0, 0, 0)),
            pl.BlockSpec((slots, share), lambda i: (0, 0)),
        ),
        scratch_shapes=[
            pltpu.VMEM((width, (heads + 2) * hd), BF16),
            pltpu.VMEM(w_out.shape, BF16),
            pltpu.VMEM((heads, tile, hd), BF16),
            pltpu.VMEM((rows, hd), BF16),
            pltpu.VMEM((rows, hd), BF16),
            pltpu.VMEM((rows, heads * qb), F32),
            pltpu.VMEM((heads, rows, hd), F32),
            pltpu.SemaphoreType.DMA((width // chunk, 3)),
            pltpu.SemaphoreType.DMA,
        ],
        compiler_params=pltpu.CompilerParams(
            dimension_semantics=("arbitrary",), vmem_limit_bytes=60 * 1024 * 1024
        ),
    )(
        seq_starts, seq_lengths, tokens, norm_gain,
        w_query, w_key, w_value, w_out, cos, sin,
    )
    nseq = episode_ids.shape[0]
    episodes = max(1, nseq // (2 * WAYS))
    classes = episodes * WAYS
    dma = pltpu.SemaphoreType.DMA
    pieces = 2 if share % 256 == 0 else 1
    fold = 2 if nseq <= 64 else 1
    dims = (n_dp, n_mp, slots, share, nseq, pieces, fold)
    every, gram = pl.pallas_call(
        functools.partial(exchange_kernel, dims),
        out_shape=(
            jax.ShapeDtypeStruct((nseq, share), F32),
            jax.ShapeDtypeStruct((nseq, nseq), F32),
        ),
        in_specs=[vmem, vmem, smem],
        out_specs=(vmem, vmem),
        scratch_shapes=[
            pltpu.VMEM((n_mp - 1, pieces, slots, share // pieces), F32),
            pltpu.VMEM((pieces, nseq, share // pieces), F32),
            pltpu.VMEM((n_mp, nseq // fold, nseq * fold), F32),
            dma((pieces, n_mp - 1)), dma((pieces, n_mp - 1)),
            dma((pieces, n_dp - 1)), dma((pieces, n_dp - 1)),
            dma((n_mp - 1,)), dma((n_mp - 1,)),
        ],
        compiler_params=pltpu.CompilerParams(collective_id=0, has_side_effects=True),
    )(head_part, token_sums, seq_lengths)
    return pl.pallas_call(
        functools.partial(score_kernel, (slots, width, nseq, classes)),
        out_shape=(
            jax.ShapeDtypeStruct((slots, WAYS), F32),
            jax.ShapeDtypeStruct((classes, share), F32),
        ),
        in_specs=[vmem] * 5,
        out_specs=(vmem, vmem),
        scratch_shapes=[pltpu.VMEM((nseq, nseq), F32)],
    )(
        every, gram,
        episode_ids.reshape(1, nseq), class_ids.reshape(1, nseq), query_flags.reshape(1, nseq),
    )


def solution(mesh):
    placed = (
        P("dp", None), P(), P(None, "mp"), P(None, "mp"), P(None, "mp"), P("mp", None),
        P("dp"), P("dp"), P(), P(), P(),
    )
    return jax.shard_map(
        functools.partial(per_device, mesh.shape["dp"], mesh.shape["mp"]),
        mesh=mesh,
        in_specs=placed,
        out_specs=(P("dp", None), P(None, "mp")),
        check_vma=False,
    )
```
